128 devices in a mesh: row: 8 (over y, core), col: 16 (over z, x).
Axes of the slice: x: 4, y: 4, z: 4, core: 2. Of those that a mesh axis runs over, the one named last changes fastest.
Arguments:
- activations: bfloat16 [8192, 7168], P('col', 'row'), may hold values from -6 to 6
- running_factor: float32 [7168, 7168], P('row', 'col'), as said below
- deltas: bfloat16 [64, 7168, 256], P('col', 'row'), may hold values from -1.5 to 1.5
- samples: int32 [64], P('col'), may hold values from 1 to 64
Outputs:
- updated_factor: float32 [7168, 7168], P('row', 'col')
- panel_factor: float32 [7168, 1024], P('row', 'col')
- solved_slab: float32 [7168, 256], P('row', 'col')
The draws below stay inside these ranges and needn't reach their ends.
Inputs may be any that keep to these rules, and one draw needn't show every extreme that they name: running_factor is symmetric and its smallest eigenvalue is 0.5 or more.
All inputs are finite; a program needn't handle non-finite values.
Results may differ from the reference program's by a relative error of at most 0.0003.
Values may be sent and summed in bfloat16 or wider, within the bound.
No kernel may reach another device: no remote copies, remote signals or barrier semaphores. Data moves between devices by JAX's collectives and lax.ppermute only.
A program may use at most 128 MiB of HBM per device.

```python
import math
import jax
import jax.numpy as jnp
from jax import lax

WIDTH = 7168
TILE = 64
PANEL = 512
PANELS = 2
SLAB = 256
SHOTS = 64
TOKENS = 8192
CLIENTS = 64
N_ROW = 8
N_COL = 16


def draw_activations(key, part):
    noise_key = jax.random.fold_in(key, 101)
    sign_key = jax.random.fold_in(key, 103)
    size_key = jax.random.fold_in(key, 107)
    shape_key = jax.random.fold_in(key, 109)
    signs = jnp.where(jax.random.bernoulli(sign_key, 0.5, (TOKENS,)), 1.0, -1.0).astype(jnp.float32)
    noise = jax.random.normal(noise_key, (TOKENS, WIDTH), jnp.float32)
    strength = signs * jax.random.uniform(size_key, (TOKENS,), jnp.float32, 0.7, 1.3)
    direction = 1.0 + 0.5 * jax.random.normal(shape_key, (WIDTH,), jnp.float32)
    values = noise + 1.5 * strength[:, None] * direction[None, :]
    return jnp.clip(values, -6.0, 6.0).astype(jnp.bfloat16)


def draw_running_factor(key, part):
    diag_key = jax.random.fold_in(key, 11)
    noise_key = jax.random.fold_in(key, 23)
    diagonal = jax.random.uniform(diag_key, (WIDTH,), jnp.float32, 1.0, 2.0)
    noise = jax.random.normal(noise_key, (WIDTH, WIDTH), jnp.float32)
    canon = (noise + noise.T) * (0.25 / math.sqrt(2.0 * WIDTH)) + jnp.diag(diagonal)
    by_rows = jnp.swapaxes(canon.reshape(-1, N_ROW, TILE, WIDTH), 0, 1).reshape(WIDTH, WIDTH)
    by_cols = jnp.swapaxes(by_rows.reshape(WIDTH, -1, N_COL, TILE), 1, 2).reshape(WIDTH, WIDTH)
    return by_cols


def with_ends(values, key, least, top_value):
    longest = values.shape.index(max(values.shape))
    spots = []
    for shift in (0, 1):
        where = [jax.random.randint(jax.random.fold_in(key, axis), (), 0, length) for axis, length in enumerate(values.shape)]
        where[longest] = (where[longest] + shift) % values.shape[longest]
        spots.append(tuple(where))
    return values.at[spots[0]].set(least).at[spots[1]].set(top_value)


def spiked(result, stream_key, source, target, parts, factor):
    def block_of(position):
        return (jnp.arange(result.shape[position]) // (result.shape[position] // parts)).reshape((-1,) + (1,) * (result.ndim - 1 - position))

    near = jax.random.permutation(stream_key, parts)[block_of(target)]
    second = (block_of(target) + parts // 2) % parts
    return jnp.where((block_of(source) == near) | (block_of(source) == second), factor * result, result)


def shard_levels(key, shape, shards, least, top_value):
    factor_of, own = 1.0, jax.random.fold_in(key, 6)
    for dim, blocks in shards:
        draws = jnp.exp(jax.random.uniform(jax.random.fold_in(own, dim), (blocks,), jnp.float32, least / len(shards), top_value / len(shards)))
        factor_of = factor_of * jnp.repeat(draws, shape[dim] // blocks).reshape([-1 if axis == dim else 1 for axis in range(len(shape))])
    return factor_of


def bell_draw_with(key, extent, spread, reach, split, heavy, held_as=jnp.bfloat16):
    entries = spread * jax.random.normal(key, extent, jnp.float32)
    if split:
        entries = entries * shard_levels(key, extent, split, -0.22, 0.18)
    return jnp.clip(spiked(entries, jax.random.fold_in(key, 3), *heavy), -reach, reach).astype(held_as)


def setup_inputs(seed: int = 0) -> dict:
    key_list = jax.random.split(jax.random.key(seed), 5)
    activations = draw_activations(jax.random.fold_in(key_list[4], 71), 0)
    running_factor = draw_running_factor(jax.random.fold_in(key_list[4], 71), 0)
    deltas = bell_draw_with(key_list[2], (CLIENTS, WIDTH, SLAB), 0.25, 1.5, ((0, 16), (1, 8)), (0, 2, 16, 2.0))
    samples = with_ends(jax.random.randint(key_list[3], (CLIENTS,), 1, SHOTS + 1), jax.random.fold_in(key_list[3], 1), 1, SHOTS).astype(jnp.int32)
    return {"activations": activations, "running_factor": running_factor, "deltas": deltas, "samples": samples}


DECAY = 0.75
DAMPING = 0.05

def canon_rows(stored, group_size):
    trailing_shape = stored.shape[1:]
    blocks = stored.reshape((group_size, -1, TILE) + trailing_shape)
    return jnp.swapaxes(blocks, 0, 1).reshape((-1,) + trailing_shape)

def store_rows(canon, group_size):
    trailing_shape = canon.shape[1:]
    blocks = canon.reshape((-1, group_size, TILE) + trailing_shape)
    return jnp.swapaxes(blocks, 0, 1).reshape((-1,) + trailing_shape)

def reference(activations, running_factor, deltas, samples):
    highest = lax.Precision.HIGHEST
    features = canon_rows(activations.T, N_ROW).astype(jnp.float32)
    previous = canon_rows(canon_rows(running_factor, N_ROW).T, N_COL).T
    token_count = activations.shape[0]
    gram_full = jnp.dot(features, features.T, precision=highest)
    factor = DECAY * previous + (1.0 - DECAY) / token_count * gram_full + DAMPING * jnp.eye(WIDTH, dtype=jnp.float32)
    columns = []
    for panel_num in range(PANELS):
        first_row = panel_num * PANEL
        diag_block = factor[first_row:first_row + PANEL, first_row:first_row + PANEL]
        lower_part = jnp.linalg.cholesky(diag_block)
        below = lax.linalg.triangular_solve(lower_part, factor[first_row:, first_row:first_row + PANEL], left_side=False, lower=True, transpose_a=True)
        column = jnp.concatenate([jnp.zeros((first_row, PANEL), jnp.float32), below], 0)
        factor = factor - jnp.dot(column, column.T, precision=highest)
        columns.append(column)
    panel_full = jnp.concatenate(columns, 1)
    weights = samples.astype(jnp.float32) / SHOTS
    moved = canon_rows(jnp.moveaxis(deltas, 1, 0), N_ROW).astype(jnp.float32)
    slab_sum = jnp.einsum('mkn,k->mn', moved, weights, precision=highest)
    done_rows = PANELS * PANEL
    head = lax.linalg.triangular_solve(panel_full[:done_rows], slab_sum[:done_rows], left_side=True, lower=True)
    remainder = slab_sum[done_rows:] - jnp.dot(panel_full[done_rows:], head, precision=highest)
    solved = jnp.concatenate([head, remainder], 0)
    factor_out = store_rows(store_rows(factor, N_ROW).T, N_COL).T
    return (factor_out, store_rows(panel_full, N_ROW), store_rows(solved, N_ROW))
```

```python
import jax
import jax.numpy as jnp
from jax import lax
from jax.experimental import pallas as pl
from jax.experimental.pallas import tpu as pltpu
from jax.sharding import Mesh
from jax.sharding import PartitionSpec as P

TILE = 64
SHOTS = 64
LEAD = 1024
DECAY = 0.75
DAMPING = 0.05
COL = ("col_0", "col_1")
ROW = ("row_y", "row_k")
ALL = ROW + COL

B=128
DEPTH=2
def mm(a,b,dims=(((1,),(0,)),((),()))):
    return lax.dot_general(a,b,dims,precision=lax.Precision.HIGHEST,preferred_element_type=jnp.float32)

def eliminate(tiles, lane):
    n=len(tiles)
    sub=lax.broadcasted_iota(jnp.int32,(8,128),0)
    def bc(x,j): return jnp.broadcast_to(x[:, j:j+1],(8,128))
    def rowb(x,i): return jnp.broadcast_to(x[i:i+1,:],(8,128))
    cols={}
    for j in range(min(DEPTH,B)):
        cols[j]={t:bc(tiles[t],j) for t in range(j//8,n)}
    for j in range(B):
        t0,s0=j//8,j%8
        jn=j+DEPTH
        if jn<B:
            cols[jn]={t:bc(tiles[t],jn) for t in range(t0,n)}
        C=cols.pop(j)
        piv=rowb(C[t0],s0)
        rinv=1.0/piv
        M={t:C[t]*rinv for t in range(t0,n)}
        below=sub>s0
        for jj in range(j+1,min(jn,B-1)+1):
            cj=cols[jj]
            f=rowb(cj[t0],s0)
            new={}
            for t in range(t0,n):
                if t<jj//8 and t!=t0: pass
                v=cj[t]-M[t]*f
                if t==t0: v=jnp.where(below,v,cj[t])
                new[t]=v
            cols[jj]={t:v for t,v in new.items()}
        row=rowb(tiles[t0],s0)
        row=jnp.where(lane==j,1.0,row)
        for t in range(t0,n):
            v=jnp.where(lane==j,0.0,tiles[t])-M[t]*row
            if t==t0: v=jnp.where(below,v,tiles[t])
            tiles[t]=v
    return tiles

def kernel(parts_ref, out_ref, w_ref, d_ref):
    lane8=lax.broadcasted_iota(jnp.int32,(8,128),1)
    lane=lax.broadcasted_iota(jnp.int32,(256,128),1)
    for q in range(4):
        def asm(i,_):
            r0=pl.ds(i*256,256)
            lo=parts_ref[2*q,r0,:]; hi=parts_ref[2*q+1,r0,:]
            w_ref[r0,q*128:(q+1)*128]=jnp.where(lane<64,lo,pltpu.roll(hi,64,1))
            w_ref[r0,512+q*128:512+(q+1)*128]=jnp.where(lane<64,pltpu.roll(lo,64,1),hi)
            return 0
        lax.fori_loop(0,4,asm,0)
    out_ref[...]=jnp.zeros_like(out_ref)
    r=lax.broadcasted_iota(jnp.int32,(128,128),0)
    c=lax.broadcasted_iota(jnp.int32,(128,128),1)
    eye=(r==c)
    colidx=lax.broadcasted_iota(jnp.int32,(128,1024),1)//128
    def step(k,_):
        k0=pl.multiple_of(k*128,128)
        ks=pl.ds(k0,128)
        blk=w_ref[ks,ks]
        tiles=[blk[8*t:8*t+8,:] for t in range(16)]
        tiles=eliminate(tiles,lane8)
        W=jnp.concatenate(tiles,0)
        dg=jnp.sum(jnp.where(eye,W,0.0),axis=1,keepdims=True)
        rs=lax.rsqrt(dg)
        li=jnp.where(eye,1.0,jnp.where(r>c,W,0.0))*rs
        d_ref[...]=li
        R=mm(li,w_ref[ks,:])
        w_ref[ks,:]=R
        w_ref[ks,ks]=li
        def upd(i,_):
            i0=pl.multiple_of(i*128,128)
            isl=pl.ds(i0,128)
            lp=mm(w_ref[isl,ks],d_ref[...],(((1,),(1,)),((),())))
            w_ref[isl,ks]=jnp.zeros((128,128),jnp.float32)
            w_ref[isl,:]=w_ref[isl,:]-mm(lp,w_ref[ks,:])
            return 0
        lax.fori_loop(k+1,8,upd,0)
        out_ref[ks,:]=jnp.where(colidx<=k,w_ref[ks,:],0.0)
        return 0
    lax.fori_loop(0,8,step,0)

def inv_chol(parts):
    return pl.pallas_call(kernel,out_shape=jax.ShapeDtypeStruct((1024,1024),jnp.float32),
        in_specs=[pl.BlockSpec(memory_space=pltpu.VMEM)],
        out_specs=pl.BlockSpec(memory_space=pltpu.VMEM),
        scratch_shapes=[pltpu.VMEM((1024,1024),jnp.float32),pltpu.VMEM((128,128),jnp.float32)],
        cost_estimate=pl.CostEstimate(flops=40_000_000_000,bytes_accessed=8_000_000,transcendentals=0),
        compiler_params=pltpu.CompilerParams(vmem_limit_bytes=40*1024*1024),
        name="inv_chol")(parts)


def permuted(x, axes, sizes, target):
    total = 1
    for s in sizes:
        total *= s
    return lax.ppermute(x, axes, [(i, target(i)) for i in range(total)])


def column_features(mine, row, col):
    tokens, width = mine.shape
    pairs = mine.reshape(tokens, -1, 2, TILE)
    halves = [pairs[:, :, h, :].reshape(tokens, width // 2) for h in range(2)]
    odd = col % 2 == 1
    first = jnp.where(odd, halves[1], halves[0])
    second = jnp.where(odd, halves[0], halves[1])

    def to(swap):
        def target(i):
            s, c = i // 16, i % 16
            h = (c % 2) ^ swap
            return (c // 2) * 16 + s + 8 * h
        return target

    got = [permuted(x, ALL, (4, 2, 4, 4), to(swap)) for swap, x in enumerate((first, second))]
    high = col // 8 == 1
    own = jnp.concatenate(
        [jnp.where(high, got[1], got[0]), jnp.where(high, got[0], got[1])], 0
    )
    y, k = row // 2, row % 2
    blocks = [own]
    for shift in (1, 3, 2):
        blocks.append(lax.ppermute(own, "row_y", [(i, (i - shift) % 4) for i in range(4)]))
    ys = [y, (y + 1) % 4, (y + 3) % 4, (y + 2) % 4]
    out = jnp.zeros((8, 2 * tokens, width // 2), mine.dtype)
    for block, at in zip(blocks, ys):
        other = lax.ppermute(block, "row_k", [(0, 1), (1, 0)])
        out = lax.dynamic_update_index_in_dim(out, block, at * 2 + k, 0)
        out = lax.dynamic_update_index_in_dim(out, other, at * 2 + 1 - k, 0)
    return out.reshape(16 * tokens, width // 2)


def dot0(left, right):
    return lax.dot_general(
        left, right, (((0,), (0,)), ((), ())), preferred_element_type=jnp.float32
    )


def dot0_high(left, right):
    return lax.dot_general(
        left, right, (((0,), (0,)), ((), ())), precision=lax.Precision.HIGHEST
    )


def dot_high(left, right):
    return jnp.dot(left, right, precision=lax.Precision.HIGHEST)


def on_device(activations, running, deltas, samples):
    row = lax.axis_index(ROW)
    col = lax.axis_index(COL)
    rows, cols = running.shape
    row_local = jnp.arange(rows, dtype=jnp.int32)
    col_local = jnp.arange(cols, dtype=jnp.int32)
    row_global = (row_local // TILE * 8 + row) * TILE + row_local % TILE
    col_global = (col_local // TILE * 16 + col) * TILE + col_local % TILE

    x_lead = lax.all_gather(activations[:, :128], COL, axis=0, tiled=True)
    tokens = x_lead.shape[0]
    scale = (1.0 - DECAY) / tokens
    y_lead = column_features(activations[:, :128], row, col)

    same = (row_global[None, :128] == col_global[:TILE, None]).astype(jnp.float32)
    lead_t = DECAY * running[:128, :TILE].T + scale * dot0(y_lead, x_lead) + DAMPING * same
    parts = lax.all_gather(lead_t, ALL, axis=0, tiled=True).reshape(8, LEAD, 128)

    rest, _ = lax.optimization_barrier((activations[:, 128:], lead_t))
    x_rest = lax.all_gather(rest, COL, axis=0, tiled=True)
    y_rest = column_features(activations[:, 128:], row, col)

    weights = samples.astype(jnp.float32) / SHOTS
    partial_t = jnp.einsum("k,kmn->nm", weights.astype(jnp.bfloat16), deltas,
                           preferred_element_type=jnp.float32)
    slab_t = lax.psum_scatter(partial_t, COL, scatter_dimension=0, tiled=True)
    slab_lead = lax.all_gather(slab_t[:, :128], ROW, axis=0)
    slab_lead = slab_lead.reshape(8, 16, 2, TILE).transpose(1, 2, 0, 3).reshape(16, LEAD)

    inverse = inv_chol(parts)

    y_all = jnp.concatenate([y_lead, y_rest], 1)
    diag_lead = (row_global[:128, None] == col_global[None, :]).astype(jnp.float32)
    top = DECAY * running[:128] + scale * dot0(x_lead, y_all) + DAMPING * diag_lead
    e_col = lax.all_gather(top, ROW, axis=0)
    e_col = e_col.reshape(8, 2, TILE, cols).swapaxes(0, 1).reshape(LEAD, cols)

    x_all = jnp.concatenate([x_lead, x_rest], 1)
    diag_t = (row_global[None, :] == col_global[:TILE, None]).astype(jnp.float32)
    e_mine = DECAY * running[:, :TILE].T + scale * dot0(y_lead, x_all) + DAMPING * diag_t
    e_row = lax.all_gather(e_mine, COL, axis=0, tiled=True)

    diag = (row_global[:, None] == col_global[None, :]).astype(jnp.float32)
    factor = DECAY * running + scale * dot0(x_all, y_all) + DAMPING * diag

    late = jnp.arange(LEAD, dtype=jnp.int32)[:, None] >= 512
    panel_col = dot_high(inverse, e_col)
    panel_col = jnp.where(late & (col_global < 512)[None, :], 0.0, panel_col)
    panel_row = dot_high(inverse, e_row)
    panel_row = jnp.where(late & (row_global < 512)[None, :], 0.0, panel_row)
    updated = factor - dot0_high(panel_row, panel_col)
    panel_out = lax.dynamic_slice_in_dim(panel_row, col * TILE, TILE, 0).T

    head = lax.dot_general(slab_lead, inverse, (((1,), (1,)), ((), ())),
                           precision=lax.Precision.HIGHEST)
    own_head = lax.dynamic_index_in_dim(
        head.reshape(16, 2, 8, TILE), row, 2, keepdims=False
    ).reshape(16, 128)
    solved = slab_t[:, 128:] - dot_high(head, panel_row[:, 128:])
    solved = jnp.concatenate([own_head, solved], 1).T
    return updated, panel_out, solved


def solution(mesh):
    finer = Mesh(mesh.devices.reshape(4, 2, 4, 4), ("row_y", "row_k", "col_0", "col_1"))
    return jax.shard_map(
        on_device,
        mesh=finer,
        in_specs=(P(COL, ROW), P(ROW, COL), P(COL, ROW, None), P(COL)),
        out_specs=(P(ROW, COL), P(ROW, COL), P(ROW, COL)),
        check_vma=False,
    )
```

```python
import jax
import jax.numpy as jnp
from jax import lax
from jax.experimental import pallas as pl
from jax.experimental.layout import Layout, with_layout_constraint
from jax.experimental.pallas import tpu as pltpu
from jax.sharding import Mesh
from jax.sharding import PartitionSpec as P

TILE = 64
SHOTS = 64
LEAD = 1024
DECAY = 0.75
DAMPING = 0.05
COL = ("col_0", "col_1")
ROW = ("row_y", "row_k")
ALL = ROW + COL
B = 128
DEPTH = 2
SPLIT = 512
VMEM = pl.BlockSpec(memory_space=pltpu.VMEM)
SMEM = pl.BlockSpec(memory_space=pltpu.SMEM)


def mm(a,b,dims=(((1,),(0,)),((),()))):
    return lax.dot_general(a,b,dims,precision=lax.Precision.HIGHEST,preferred_element_type=jnp.float32)

def eliminate(tiles, lane):
    n=len(tiles)
    sub=lax.broadcasted_iota(jnp.int32,(8,128),0)
    def bc(x,j): return jnp.broadcast_to(x[:, j:j+1],(8,128))
    def rowb(x,i): return jnp.broadcast_to(x[i:i+1,:],(8,128))
    cols={}
    for j in range(min(DEPTH,B)):
        cols[j]={t:bc(tiles[t],j) for t in range(j//8,n)}
    for j in range(B):
        t0,s0=j//8,j%8
        jn=j+DEPTH
        if jn<B:
            cols[jn]={t:bc(tiles[t],jn) for t in range(t0,n)}
        C=cols.pop(j)
        piv=rowb(C[t0],s0)
        rinv=1.0/piv
        M={t:C[t]*rinv for t in range(t0,n)}
        below=sub>s0
        for jj in range(j+1,min(jn,B-1)+1):
            cj=cols[jj]
            f=rowb(cj[t0],s0)
            new={}
            for t in range(t0,n):
                if t<jj//8 and t!=t0: pass
                v=cj[t]-M[t]*f
                if t==t0: v=jnp.where(below,v,cj[t])
                new[t]=v
            cols[jj]={t:v for t,v in new.items()}
        row=rowb(tiles[t0],s0)
        row=jnp.where(lane==j,1.0,row)
        for t in range(t0,n):
            v=jnp.where(lane==j,0.0,tiles[t])-M[t]*row
            if t==t0: v=jnp.where(below,v,tiles[t])
            tiles[t]=v
    return tiles


def assemble(pos_ref, own_ref, other_ref, w_ref):
    lane = lax.broadcasted_iota(jnp.int32, (256, B), 1)
    y, k = pos_ref[0], pos_ref[1]
    north = k == 0
    for q in range(4):
        ahead = lax.rem(q - y + 4, 4)

        def place(i, _):
            at = pl.ds(pl.multiple_of(i * 256, 256), 256)
            mine, theirs = own_ref[ahead, at, :], other_ref[ahead, at, :]
            low = jnp.where(north, mine, theirs)
            high = jnp.where(north, theirs, mine)
            w_ref[at, q * B : (q + 1) * B] = jnp.where(lane < 64, low, pltpu.roll(high, 64, 1))
            w_ref[at, 512 + q * B : 512 + (q + 1) * B] = jnp.where(
                lane < 64, pltpu.roll(low, 64, 1), high
            )
            return 0

        lax.fori_loop(0, 4, place, 0)


def factor_steps(w_ref, d_ref, first, last):
    lane8 = lax.broadcasted_iota(jnp.int32, (8, B), 1)
    r = lax.broadcasted_iota(jnp.int32, (B, B), 0)
    c = lax.broadcasted_iota(jnp.int32, (B, B), 1)

    def step(k, _):
        ks = pl.ds(pl.multiple_of(k * B, B), B)
        block = w_ref[ks, ks]
        tiles = eliminate([block[8 * t : 8 * t + 8, :] for t in range(B // 8)], lane8)
        whole = jnp.concatenate(tiles, 0)
        pivots = jnp.sum(jnp.where(r == c, whole, 0.0), axis=1, keepdims=True)
        inverse = jnp.where(r == c, 1.0, jnp.where(r > c, whole, 0.0)) * lax.rsqrt(pivots)
        d_ref[...] = inverse
        w_ref[ks, :] = mm(inverse, w_ref[ks, :])
        w_ref[ks, ks] = inverse

        def update(i, _):
            at = pl.ds(pl.multiple_of(i * B, B), B)
            left = mm(w_ref[at, ks], d_ref[...], (((1,), (1,)), ((), ())))
            w_ref[at, ks] = jnp.zeros((B, B), jnp.float32)
            w_ref[at, :] = w_ref[at, :] - mm(left, w_ref[ks, :])
            return 0

        lax.fori_loop(k + 1, 8, update, 0)
        return 0

    lax.fori_loop(first, last, step, 0)


def first_kernel(pos_ref, own_ref, other_ref, w_ref, d_ref):
    assemble(pos_ref, own_ref, other_ref, w_ref)
    factor_steps(w_ref, d_ref, 0, 4)


def second_kernel(in_ref, w_ref, d_ref):
    w_ref[...] = in_ref[...]
    factor_steps(w_ref, d_ref, 4, 8)
    block = lax.broadcasted_iota(jnp.int32, (B, LEAD), 1) // B
    for k in range(8):
        w_ref[k * B : (k + 1) * B, :] = jnp.where(block <= k, w_ref[k * B : (k + 1) * B, :], 0.0)


def factor_call(body, inputs, specs, name):
    return pl.pallas_call(
        body,
        out_shape=jax.ShapeDtypeStruct((LEAD, LEAD), jnp.float32),
        in_specs=specs,
        out_specs=VMEM,
        scratch_shapes=[pltpu.VMEM((B, B), jnp.float32)],
        cost_estimate=pl.CostEstimate(
            flops=20_000_000_000, bytes_accessed=8_000_000, transcendentals=0
        ),
        compiler_params=pltpu.CompilerParams(vmem_limit_bytes=40 * 1024 * 1024),
        name=name,
    )(*inputs)


def gram_kernel(pos_ref, x_ref, *refs):
    own, other, out_ref, held = refs[:4], refs[4:8], refs[8], refs[9]
    step = pl.program_id(0)
    for d in range(4):

        @pl.when(step == d)
        def _():
            held[0] = own[d][...]
            held[1] = other[d][...]

    k = pos_ref[1]
    total = jnp.dot(held[0], x_ref[0, k], preferred_element_type=jnp.float32)
    total += jnp.dot(held[1], x_ref[0, 1 - k], preferred_element_type=jnp.float32)

    @pl.when(step == 0)
    def _():
        out_ref[...] = total

    @pl.when(step > 0)
    def _():
        out_ref[...] += total


def gram(pos, x, own, other):
    feats, block = own[0].shape
    width = x.shape[-1]
    whole = pl.BlockSpec((feats, block), lambda i, pos: (0, 0))
    return pl.pallas_call(
        gram_kernel,
        out_shape=jax.ShapeDtypeStruct((feats, width), jnp.float32),
        grid_spec=pltpu.PrefetchScalarGridSpec(
            num_scalar_prefetch=1,
            grid=(4,),
            in_specs=[
                pl.BlockSpec(
                    (1, 2, block, width), lambda i, pos: (lax.rem(pos[0] + i, 4), 0, 0, 0)
                )
            ]
            + [whole] * 8,
            out_specs=pl.BlockSpec((feats, width), lambda i, pos: (0, 0)),
            scratch_shapes=[pltpu.VMEM((2, feats, block), jnp.bfloat16)],
        ),
        cost_estimate=pl.CostEstimate(
            flops=6_600_000_000, bytes_accessed=24_000_000, transcendentals=0
        ),
        compiler_params=pltpu.CompilerParams(vmem_limit_bytes=48 * 1024 * 1024),
        name="gram",
    )(pos, x, *own, *other)


def triangular_product(pos_ref, inv_ref, held, out_ref, masked):
    width = out_ref.shape[1]
    lane = lax.broadcasted_iota(jnp.int32, (B, width), 1)
    for i in range(8):
        depth = (i + 1) * B
        value = mm(inv_ref[i * B : depth, :depth], held[:depth, :])
        if i >= 4:
            value = jnp.where((lane < TILE) & masked, 0.0, value)
        out_ref[i * B : depth, :] = value


def panel_col_kernel(pos_ref, inv_ref, *refs):
    own, other, out_ref, held = refs[:4], refs[4:8], refs[8], refs[9]
    y, k = pos_ref[0], pos_ref[1]
    for d in range(4):
        for piece, side in ((own[d], k), (other[d], 1 - k)):
            row = lax.rem(y + d, 4) * 2 + side
            for t in range(2):
                at = pl.ds(pl.multiple_of(t * 512 + row * TILE, TILE), TILE)
                held[at, :] = piece[t * TILE : (t + 1) * TILE, :]
    triangular_product(pos_ref, inv_ref, held, out_ref, pos_ref[2] < 2)


def panel_row_kernel(pos_ref, inv_ref, *refs):
    left, right, out_ref, held = refs[:4], refs[4:8], refs[8], refs[9]
    z, x = pos_ref[2], pos_ref[3]
    for i in range(4):
        for j in range(4):
            col = lax.rem(z + i, 4) * 4 + lax.rem(x + j, 4)
            at = pl.ds(pl.multiple_of(col * TILE, TILE), TILE)
            held[at, :SPLIT] = left[i][j]
            held[at, SPLIT:] = right[j][i]
    triangular_product(pos_ref, inv_ref, held, out_ref, True)


def panel_call(body, pos, inverse, pieces, width, name):
    return pl.pallas_call(
        body,
        out_shape=jax.ShapeDtypeStruct((LEAD, width), jnp.float32),
        in_specs=[SMEM] + [VMEM] * (1 + len(pieces)),
        out_specs=VMEM,
        scratch_shapes=[pltpu.VMEM((LEAD, width), jnp.float32)],
        cost_estimate=pl.CostEstimate(
            flops=LEAD * LEAD * width * 6, bytes_accessed=12_000_000, transcendentals=0
        ),
        compiler_params=pltpu.CompilerParams(vmem_limit_bytes=40 * 1024 * 1024),
        name=name,
    )(pos, inverse, *pieces)


def fetch(x, axis, ahead):
    size = lax.axis_size(axis)
    return lax.ppermute(x, axis, [(i, (i - ahead) % size) for i in range(size)])


def fetch_each(x, axis):
    return [x] + [fetch(x, axis, ahead) for ahead in (1, 2, 3)]


def swap(x):
    return fetch(x, "row_k", 1)


def copy_for_each(x, axes, size):
    return lax.all_to_all(jnp.broadcast_to(x[None], (size, *x.shape)), axes, 0, 0, tiled=True)


def scattered_sum(x, axis):
    me = lax.axis_index(axis)
    total = lax.dynamic_index_in_dim(x, me, 0, keepdims=False)
    for ahead in (1, 2, 3):
        part = lax.dynamic_index_in_dim(x, (me - ahead) % 4, 0, keepdims=False)
        total = total + fetch(part, axis, ahead)
    return total


def own_column_features(activations, row, col):
    tokens, width = activations.shape
    turned = activations.T.reshape(-1, 2, TILE, tokens)
    halves = [turned[:, h].reshape(width // 2, tokens) for h in range(2)]
    odd = col % 2 == 1
    sent = (jnp.where(odd, halves[1], halves[0]), jnp.where(odd, halves[0], halves[1]))

    def pairs(other):
        found = []
        for i in range(128):
            s, c = i // 16, i % 16
            found.append((i, (c // 2) * 16 + s + 8 * ((c % 2) ^ other)))
        return found

    got = [lax.ppermute(x, ALL, pairs(other)) for other, x in enumerate(sent)]
    high = col // 8 == 1
    return jnp.concatenate(
        [jnp.where(high, got[1], got[0]), jnp.where(high, got[0], got[1])], 1
    )


def dot0(left, right):
    return lax.dot_general(
        left, right, (((0,), (0,)), ((), ())), preferred_element_type=jnp.float32
    )


def dot0_high(left, right):
    return lax.dot_general(
        left, right, (((0,), (0,)), ((), ())), precision=lax.Precision.HIGHEST
    )


def on_device(activations, running, deltas, samples):
    y, k = lax.axis_index("row_y"), lax.axis_index("row_k")
    z, x = lax.axis_index("col_0"), lax.axis_index("col_1")
    row, col = y * 2 + k, z * 4 + x
    pos = jnp.stack([y, k, z, x]).astype(jnp.int32)
    rows, cols = running.shape
    row_local = jnp.arange(rows, dtype=jnp.int32)
    col_local = jnp.arange(cols, dtype=jnp.int32)
    row_global = (row_local // TILE * 8 + row) * TILE + row_local % TILE
    col_global = (col_local // TILE * 16 + col) * TILE + col_local % TILE

    everything = lax.all_gather(activations, COL, axis=0)
    everything = with_layout_constraint(everything, Layout((0, 1, 2)))
    tokens = everything.shape[0] * everything.shape[1]
    scale = (1.0 - DECAY) / tokens

    lead = activations[:, :128]
    lead_all = copy_for_each(lead, ROW, 8)
    partial = lax.dot_general(
        lead_all, lead, (((1,), (0,)), ((), ())), preferred_element_type=jnp.float32
    )
    partial = partial.reshape(8, 2, TILE, 128).swapaxes(0, 1).reshape(16, TILE, 128)
    lead_sum = lax.all_to_all(partial, COL, 0, 0, tiled=True).sum(0)
    same = (row_global[None, :128] == col_global[:TILE, None]).astype(jnp.float32)
    lead_t = DECAY * running[:128, :TILE].T + scale * lead_sum + DAMPING * same
    lead_cols = copy_for_each(lead_t, COL, 16).reshape(LEAD, 128)
    parts = jnp.stack(fetch_each(lead_cols, "row_y"))
    other_parts = swap(parts)

    feats = own_column_features(activations, row, col)
    feats, parts, other_parts = lax.optimization_barrier((feats, parts, other_parts))
    y_own = fetch_each(feats, "row_y")

    state = factor_call(first_kernel, (pos, parts, other_parts), [SMEM, VMEM, VMEM], "factor_a")
    y_own, deltas, state = lax.optimization_barrier((y_own, deltas, state))

    weights = (samples.astype(jnp.float32) / SHOTS).astype(jnp.bfloat16)
    partial_t = jnp.einsum(
        "k,kmn->nm", weights, deltas, preferred_element_type=jnp.float32
    )
    slab_t = scattered_sum(partial_t.reshape(4, 64, rows), "col_0")
    slab_t = scattered_sum(slab_t.reshape(4, 16, rows), "col_1")

    y_other = [swap(part) for part in y_own]
    slab_lead = fetch_each(slab_t[:, :128], "row_y")
    slab_lead = jnp.stack([jnp.stack(slab_lead), swap(jnp.stack(slab_lead))])

    by_block = everything.reshape(4, 2, tokens // 8, rows)
    gram_t = gram(pos, by_block, y_own, y_other)

    diag_t = (row_global[None, :] == col_global[:TILE, None]).astype(jnp.float32)
    e_mine = DECAY * running[:, :TILE].T + scale * gram_t[:TILE] + DAMPING * diag_t
    diag_lead = (row_global[:128, None] == col_global[None, :]).astype(jnp.float32)
    top = DECAY * running[:128] + scale * gram_t[:, :128].T + DAMPING * diag_lead
    left = jnp.stack(fetch_each(e_mine[:, :SPLIT], "col_1"))
    right = jnp.stack(fetch_each(e_mine[:, SPLIT:], "col_0"))
    top_own = fetch_each(top, "row_y")
    left, right, state = lax.optimization_barrier((left, right, state))
    left = fetch_each(left, "col_0")
    right = fetch_each(right, "col_1")
    top_other = [swap(part) for part in top_own]

    inverse = factor_call(second_kernel, (state,), [VMEM], "factor_b")

    diag = (row_global[:, None] == col_global[None, :]).astype(jnp.float32)
    factor = DECAY * running + scale * gram_t.T + DAMPING * diag

    panel_col = panel_call(panel_col_kernel, pos, inverse, top_own + top_other, cols, "panel_col")
    panel_row = panel_call(panel_row_kernel, pos, inverse, left + right, rows, "panel_row")
    updated = factor - dot0_high(panel_row, panel_col)
    panel_out = lax.dynamic_slice_in_dim(panel_row, col * TILE, TILE, 0).T

    slab_lead = jnp.where(k == 0, slab_lead, slab_lead[::-1])
    slab_lead = jnp.roll(slab_lead, y, axis=1)
    slab_lead = slab_lead.reshape(2, 4, 16, 2, TILE).transpose(2, 3, 1, 0, 4).reshape(16, LEAD)
    head = lax.dot_general(
        slab_lead, inverse, (((1,), (1,)), ((), ())), precision=lax.Precision.HIGHEST
    )
    own_head = lax.dynamic_index_in_dim(
        head.reshape(16, 2, 8, TILE), row, 2, keepdims=False
    ).reshape(16, 128)
    rest = jnp.dot(head, panel_row, precision=lax.Precision.HIGHEST)
    solved = jnp.concatenate([own_head, slab_t[:, 128:] - rest[:, 128:]], 1).T
    return updated, panel_out, solved


def solution(mesh):
    finer = Mesh(mesh.devices.reshape(4, 2, 4, 4), ("row_y", "row_k", "col_0", "col_1"))
    return jax.shard_map(
        on_device,
        mesh=finer,
        in_specs=(P(COL, ROW), P(ROW, COL), P(COL, ROW, None), P(COL)),
        out_specs=(P(ROW, COL), P(ROW, COL), P(ROW, COL)),
        check_vma=False,
    )
```

```python
import jax
import jax.numpy as jnp
from jax import lax
from jax.experimental import pallas as pl
from jax.experimental.layout import Layout, with_layout_constraint
from jax.experimental.pallas import tpu as pltpu
from jax.sharding import Mesh
from jax.sharding import PartitionSpec as P


TILE = 64
SHOTS = 64
LEAD = 1024
DECAY = 0.75
DAMPING = 0.05
COL = ("col_0", "col_1")
ROW = ("row_y", "row_k")
ALL = ROW + COL
B = 128
DEPTH = 5
FIRST = 5
SPLIT = 512
VMEM = pl.BlockSpec(memory_space=pltpu.VMEM)
SMEM = pl.BlockSpec(memory_space=pltpu.SMEM)


def mm(a,b,dims=(((1,),(0,)),((),()))):
    return lax.dot_general(a,b,dims,precision=lax.Precision.HIGHEST,preferred_element_type=jnp.float32)


def eliminate(tiles, lane):
    n=len(tiles)
    sub=lax.broadcasted_iota(jnp.int32,(8,128),0)

    def bc(x,j): return jnp.broadcast_to(x[:, j:j+1],(8,128))

    def rowb(x,i): return jnp.broadcast_to(x[i:i+1,:],(8,128))

    cols={}
    for j in range(min(DEPTH,B)):
        cols[j]={t:bc(tiles[t],j) for t in range(j//8,n)}
    for j in range(B):
        t0,s0=j//8,j%8
        jn=j+DEPTH
        if jn<B:
            cols[jn]={t:bc(tiles[t],jn) for t in range(t0,n)}
        C=cols.pop(j)
        piv=rowb(C[t0],s0)
        rinv=1.0/piv
        M={t:C[t]*rinv for t in range(t0,n)}
        below=sub>s0
        for jj in range(j+1,min(jn,B-1)+1):
            cj=cols[jj]
            f=rowb(cj[t0],s0)
            new={}
            for t in range(t0,n):
                v=cj[t]-M[t]*f
                if t==t0: v=jnp.where(below,v,cj[t])
                new[t]=v
            cols[jj]={t:v for t,v in new.items()}
        row=rowb(tiles[t0],s0)
        row=jnp.where(lane==j,1.0,row)
        for t in range(t0,n):
            v=jnp.where(lane==j,0.0,tiles[t])-M[t]*row
            if t==t0: v=jnp.where(below,v,tiles[t])
            tiles[t]=v
    return tiles


def assemble(pos_ref, own_ref, other_ref, w_ref):
    lane = lax.broadcasted_iota(jnp.int32, (256, B), 1)
    y, k = pos_ref[0], pos_ref[1]
    north = k == 0
    for q in range(4):
        ahead = lax.rem(q - y + 4, 4)

        def place(i, _):
            at = pl.ds(pl.multiple_of(i * 256, 256), 256)
            mine, theirs = own_ref[ahead, at, :], other_ref[ahead, at, :]
            low = jnp.where(north, mine, theirs)
            high = jnp.where(north, theirs, mine)
            w_ref[at, q * B : (q + 1) * B] = jnp.where(lane < 64, low, pltpu.roll(high, 64, 1))
            w_ref[at, 512 + q * B : 512 + (q + 1) * B] = jnp.where(
                lane < 64, pltpu.roll(low, 64, 1), high
            )
            return 0

        lax.fori_loop(0, 4, place, 0)


def factor_steps(w_ref, d_ref, left_ref, first, last):
    lane8 = lax.broadcasted_iota(jnp.int32, (8, B), 1)
    r = lax.broadcasted_iota(jnp.int32, (B, B), 0)
    c = lax.broadcasted_iota(jnp.int32, (B, B), 1)

    def step(k, _):
        ks = pl.ds(pl.multiple_of(k * B, B), B)
        block = w_ref[ks, ks]
        tiles = eliminate([block[8 * t : 8 * t + 8, :] for t in range(B // 8)], lane8)
        whole = jnp.concatenate(tiles, 0)
        pivots = jnp.sum(jnp.where(r == c, whole, 0.0), axis=1, keepdims=True)
        inverse = jnp.where(r == c, 1.0, jnp.where(r > c, whole, 0.0)) * lax.rsqrt(pivots)
        d_ref[...] = inverse
        w_ref[ks, :] = mm(inverse, w_ref[ks, :])
        w_ref[ks, ks] = inverse

        below = lax.broadcasted_iota(jnp.int32, (LEAD, B), 0) // B > k
        column = w_ref[:, ks]
        left_ref[...] = mm(
            jnp.where(below, column, 0.0), d_ref[...], (((1,), (1,)), ((), ()))
        )
        w_ref[:, ks] = jnp.where(below, 0.0, column)

        def update(i, _):
            at = pl.ds(pl.multiple_of(i * 256, 256), 256)
            w_ref[at, :] = w_ref[at, :] - mm(left_ref[at, :], w_ref[ks, :])
            return 0

        lax.fori_loop((k + 1) // 2, 4, update, 0)
        return 0

    lax.fori_loop(first, last, step, 0)


def first_kernel(pos_ref, own_ref, other_ref, w_ref, d_ref, left_ref):
    assemble(pos_ref, own_ref, other_ref, w_ref)
    factor_steps(w_ref, d_ref, left_ref, 0, FIRST)


def second_kernel(in_ref, w_ref, d_ref, left_ref):
    w_ref[...] = in_ref[...]
    factor_steps(w_ref, d_ref, left_ref, FIRST, 8)
    block = lax.broadcasted_iota(jnp.int32, (B, LEAD), 1) // B
    for k in range(8):
        w_ref[k * B : (k + 1) * B, :] = jnp.where(block <= k, w_ref[k * B : (k + 1) * B, :], 0.0)


def factor_call(body, inputs, specs):
    return pl.pallas_call(
        body,
        out_shape=jax.ShapeDtypeStruct((LEAD, LEAD), jnp.float32),
        in_specs=specs,
        out_specs=VMEM,
        scratch_shapes=[pltpu.VMEM((B, B), jnp.float32), pltpu.VMEM((LEAD, B), jnp.float32)],
        cost_estimate=pl.CostEstimate(
            flops=20_000_000_000, bytes_accessed=8_000_000, transcendentals=0
        ),
        compiler_params=pltpu.CompilerParams(vmem_limit_bytes=40 * 1024 * 1024),
    )(*inputs)


def gram_kernel(pos_ref, x_ref, *refs):
    own, other, out_ref, held = refs[:4], refs[4:8], refs[8], refs[9]
    step = pl.program_id(0)
    for d in range(4):

        @pl.when(step == d)
        def _():
            held[0] = own[d][...]
            held[1] = other[d][...]

    k = pos_ref[1]
    total = jnp.dot(held[0], x_ref[0, k], preferred_element_type=jnp.float32)
    total += jnp.dot(held[1], x_ref[0, 1 - k], preferred_element_type=jnp.float32)

    @pl.when(step == 0)
    def _():
        out_ref[...] = total

    @pl.when(step > 0)
    def _():
        out_ref[...] += total


def gram(pos, x, own, other):
    feats, block = own[0].shape
    width = x.shape[-1]
    whole = pl.BlockSpec((feats, block), lambda i, pos: (0, 0))
    return pl.pallas_call(
        gram_kernel,
        out_shape=jax.ShapeDtypeStruct((feats, width), jnp.float32),
        grid_spec=pltpu.PrefetchScalarGridSpec(
            num_scalar_prefetch=1,
            grid=(4,),
            in_specs=[
                pl.BlockSpec(
                    (1, 2, block, width), lambda i, pos: (lax.rem(pos[0] + i, 4), 0, 0, 0)
                )
            ]
            + [whole] * 8,
            out_specs=pl.BlockSpec((feats, width), lambda i, pos: (0, 0)),
            scratch_shapes=[pltpu.VMEM((2, feats, block), jnp.bfloat16)],
        ),
        cost_estimate=pl.CostEstimate(
            flops=6_600_000_000, bytes_accessed=24_000_000, transcendentals=0
        ),
        compiler_params=pltpu.CompilerParams(vmem_limit_bytes=48 * 1024 * 1024),
        name="gram",
    )(pos, x, *own, *other)


def triangular_product(inv_ref, held, out_ref, masked):
    width = out_ref.shape[1]
    lane = lax.broadcasted_iota(jnp.int32, (B, width), 1)
    for i in range(8):
        depth = (i + 1) * B
        value = mm(inv_ref[i * B : depth, :depth], held[:depth, :])
        if i >= 4:
            value = jnp.where((lane < TILE) & masked, 0.0, value)
        out_ref[i * B : depth, :] = value


def panel_col_kernel(pos_ref, inv_ref, *refs):
    own, other, out_ref, held = refs[:4], refs[4:8], refs[8], refs[9]
    y, k = pos_ref[0], pos_ref[1]
    for d in range(4):
        for piece, side in ((own[d], k), (other[d], 1 - k)):
            row = lax.rem(y + d, 4) * 2 + side
            for t in range(2):
                at = pl.ds(pl.multiple_of(t * 512 + row * TILE, TILE), TILE)
                held[at, :] = piece[t * TILE : (t + 1) * TILE, :]
    triangular_product(inv_ref, held, out_ref, pos_ref[2] < 2)


def panel_row_kernel(pos_ref, inv_ref, *refs):
    left, right, out_ref, held = refs[:4], refs[4:8], refs[8], refs[9]
    z, x = pos_ref[2], pos_ref[3]
    for i in range(4):
        for j in range(4):
            col = lax.rem(z + i, 4) * 4 + lax.rem(x + j, 4)
            at = pl.ds(pl.multiple_of(col * TILE, TILE), TILE)
            held[at, :SPLIT] = left[i][j]
            held[at, SPLIT:] = right[j][i]
    triangular_product(inv_ref, held, out_ref, True)


def panel_call(body, pos, inverse, pieces, width):
    return pl.pallas_call(
        body,
        out_shape=jax.ShapeDtypeStruct((LEAD, width), jnp.float32),
        in_specs=[SMEM] + [VMEM] * (1 + len(pieces)),
        out_specs=VMEM,
        scratch_shapes=[pltpu.VMEM((LEAD, width), jnp.float32)],
        cost_estimate=pl.CostEstimate(
            flops=LEAD * LEAD * width * 6, bytes_accessed=12_000_000, transcendentals=0
        ),
        compiler_params=pltpu.CompilerParams(vmem_limit_bytes=40 * 1024 * 1024),
    )(pos, inverse, *pieces)


def fetch(x, axis, ahead):
    size = lax.axis_size(axis)
    return lax.ppermute(x, axis, [(i, (i - ahead) % size) for i in range(size)])


def fetch_each(x, axis):
    return [x] + [fetch(x, axis, ahead) for ahead in (1, 2, 3)]


def swap(x):
    return fetch(x, "row_k", 1)


def copy_for_each(x, axes, size):
    return lax.all_to_all(jnp.broadcast_to(x[None], (size, *x.shape)), axes, 0, 0, tiled=True)


def fetch_shares(x, axis):
    me = lax.axis_index(axis)
    return [lax.dynamic_index_in_dim(x, me, 0, keepdims=False)] + [
        fetch(lax.dynamic_index_in_dim(x, (me - ahead) % 4, 0, keepdims=False), axis, ahead)
        for ahead in (1, 2, 3)
    ]


def column_features_to_send(activations, col):
    tokens, width = activations.shape
    turned = activations.T.reshape(-1, 2, TILE, tokens)
    halves = [turned[:, h].reshape(width // 2, tokens) for h in range(2)]
    odd = col % 2 == 1
    sent = [jnp.where(odd, halves[1], halves[0]), jnp.where(odd, halves[0], halves[1])]
    pairs = [[], []]
    for other in range(2):
        for i in range(128):
            s, c = i // 16, i % 16
            pairs[other].append((i, (c // 2) * 16 + s + 8 * ((c % 2) ^ other)))
    return sent, pairs


def dot0_high(left, right):
    return lax.dot_general(
        left, right, (((0,), (0,)), ((), ())), precision=lax.Precision.HIGHEST
    )


def on_device(activations, running, deltas, samples):
    y, k = lax.axis_index("row_y"), lax.axis_index("row_k")
    z, x = lax.axis_index("col_0"), lax.axis_index("col_1")
    row, col = y * 2 + k, z * 4 + x
    pos = jnp.stack([y, k, z, x]).astype(jnp.int32)
    rows, cols = running.shape
    row_local = jnp.arange(rows, dtype=jnp.int32)
    col_local = jnp.arange(cols, dtype=jnp.int32)
    row_global = (row_local // TILE * 8 + row) * TILE + row_local % TILE
    col_global = (col_local // TILE * 16 + col) * TILE + col_local % TILE

    everything = lax.all_gather(activations, COL, axis=0)
    everything = with_layout_constraint(everything, Layout((0, 1, 2)))
    tokens = everything.shape[0] * everything.shape[1]
    scale = (1.0 - DECAY) / tokens

    sent, pairs = column_features_to_send(activations, col)
    lead = activations[:, :128]
    sent, lead = lax.optimization_barrier((sent, lead))
    got = [lax.ppermute(part, ALL, pair) for part, pair in zip(sent, pairs)]

    lead_all = copy_for_each(lead, ROW, 8)
    partial = lax.dot_general(
        lead_all, lead, (((1,), (0,)), ((), ())), preferred_element_type=jnp.float32
    )
    partial = partial.reshape(8, 2, TILE, 128).swapaxes(0, 1).reshape(16, TILE, 128)
    lead_sum = lax.all_to_all(partial, COL, 0, 0, tiled=True).sum(0)
    same = (row_global[None, :128] == col_global[:TILE, None]).astype(jnp.float32)
    lead_t = DECAY * running[:128, :TILE].T + scale * lead_sum + DAMPING * same
    lead_cols = copy_for_each(lead_t, COL, 16).reshape(LEAD, 128)
    parts = jnp.stack(fetch_each(lead_cols, "row_y"))

    weights = (samples.astype(jnp.float32) / SHOTS).astype(jnp.bfloat16)
    partial_t = jnp.einsum(
        "k,kmn->nm", weights, deltas, preferred_element_type=jnp.float32
    )
    partial_t, parts = lax.optimization_barrier((partial_t, parts))
    other_parts = swap(parts)
    slab_parts = fetch_shares(partial_t.reshape(4, 64, rows), "col_0")
    high = col // 8 == 1
    feats = jnp.concatenate(
        [jnp.where(high, got[1], got[0]), jnp.where(high, got[0], got[1])], 1
    )
    feats, parts, other_parts = lax.optimization_barrier((feats, parts, other_parts))
    y_own = fetch_each(feats, "row_y")

    state = factor_call(first_kernel, (pos, parts, other_parts), [SMEM, VMEM, VMEM])
    y_own, slab_parts, state = lax.optimization_barrier((y_own, slab_parts, state))
    y_other = [swap(part) for part in y_own]
    slab_parts = fetch_shares(sum(slab_parts).reshape(4, 16, rows), "col_1")

    by_block = everything.reshape(4, 2, tokens // 8, rows)
    gram_t = gram(pos, by_block, y_own, y_other)
    slab_parts, gram_t = lax.optimization_barrier((slab_parts, gram_t))
    slab_t = sum(slab_parts)
    slab_side = jnp.stack([slab_t[:, :128], swap(slab_t[:, :128])])
    slab_lead = fetch_each(slab_side, "row_y")

    diag_t = (row_global[None, :] == col_global[:TILE, None]).astype(jnp.float32)
    e_mine = DECAY * running[:, :TILE].T + scale * gram_t[:TILE] + DAMPING * diag_t
    diag_lead = (row_global[:128, None] == col_global[None, :]).astype(jnp.float32)
    top = DECAY * running[:128] + scale * gram_t[:, :128].T + DAMPING * diag_lead
    left = jnp.stack(fetch_each(e_mine[:, :SPLIT], "col_1"))
    right = jnp.stack(fetch_each(e_mine[:, SPLIT:], "col_0"))
    top_own = fetch_each(top, "row_y")
    left, right, state = lax.optimization_barrier((left, right, state))
    left = fetch_each(left, "col_0")
    right = fetch_each(right, "col_1")
    top_other = [swap(part) for part in top_own]

    inverse = factor_call(second_kernel, (state,), [VMEM])

    diag = (row_global[:, None] == col_global[None, :]).astype(jnp.float32)
    factor = DECAY * running + scale * gram_t.T + DAMPING * diag

    panel_col = panel_call(panel_col_kernel, pos, inverse, top_own + top_other, cols)
    panel_row = panel_call(panel_row_kernel, pos, inverse, left + right, rows)
    updated = factor - dot0_high(panel_row, panel_col)
    panel_out = lax.dynamic_slice_in_dim(panel_row, col * TILE, TILE, 0).T

    slab_lead = jnp.stack(slab_lead)
    slab_lead = jnp.where(k == 0, slab_lead, slab_lead[:, ::-1])
    slab_lead = jnp.roll(slab_lead, y, axis=0)
    slab_lead = slab_lead.reshape(4, 2, 16, 2, TILE).transpose(2, 3, 0, 1, 4).reshape(16, LEAD)
    head = lax.dot_general(
        slab_lead, inverse, (((1,), (1,)), ((), ())), precision=lax.Precision.HIGHEST
    )
    own_head = lax.dynamic_index_in_dim(
        head.reshape(16, 2, 8, TILE), row, 2, keepdims=False
    ).reshape(16, 128)
    rest = jnp.dot(head, panel_row, precision=lax.Precision.HIGHEST)
    solved = jnp.concatenate([own_head, slab_t[:, 128:] - rest[:, 128:]], 1).T
    return updated, panel_out, solved


def solution(mesh):
    finer = Mesh(mesh.devices.reshape(4, 2, 4, 4), ("row_y", "row_k", "col_0", "col_1"))
    return jax.shard_map(
        on_device,
        mesh=finer,
        in_specs=(P(COL, ROW), P(ROW, COL), P(COL, ROW, None), P(COL)),
        out_specs=(P(ROW, COL), P(ROW, COL), P(ROW, COL)),
        check_vma=False,
    )
```

```python
import jax
import jax.numpy as jnp
from jax import lax
from jax.experimental import pallas as pl
from jax.experimental.layout import Layout, with_layout_constraint
from jax.experimental.pallas import tpu as pltpu
from jax.sharding import Mesh
from jax.sharding import PartitionSpec as P

TILE = 64
SHOTS = 64
LEAD = 1024
DECAY = 0.75
DAMPING = 0.05
COL = ("col_0", "col_1")
ROW = ("row_y", "row_k")
ALL = ROW + COL
B = 128
DEPTH = 5
FIRST = 4
SPLIT = 512
VMEM = pl.BlockSpec(memory_space=pltpu.VMEM)
SMEM = pl.BlockSpec(memory_space=pltpu.SMEM)


def mm(a,b,dims=(((1,),(0,)),((),()))):
    return lax.dot_general(a,b,dims,precision=lax.Precision.HIGHEST,preferred_element_type=jnp.float32)

def eliminate(tiles, lane):
    n=len(tiles)
    sub=lax.broadcasted_iota(jnp.int32,(8,128),0)
    def bc(x,j): return jnp.broadcast_to(x[:, j:j+1],(8,128))
    def rowb(x,i): return jnp.broadcast_to(x[i:i+1,:],(8,128))
    cols={}
    for j in range(min(DEPTH,B)):
        cols[j]={t:bc(tiles[t],j) for t in range(j//8,n)}
    for j in range(B):
        t0,s0=j//8,j%8
        jn=j+DEPTH
        if jn<B:
            cols[jn]={t:bc(tiles[t],jn) for t in range(t0,n)}
        C=cols.pop(j)
        piv=rowb(C[t0],s0)
        rinv=1.0/piv
        M={t:C[t]*rinv for t in range(t0,n)}
        below=sub>s0
        for jj in range(j+1,min(jn,B-1)+1):
            cj=cols[jj]
            f=rowb(cj[t0],s0)
            new={}
            for t in range(t0,n):
                if t<jj//8 and t!=t0: pass
                v=cj[t]-M[t]*f
                if t==t0: v=jnp.where(below,v,cj[t])
                new[t]=v
            cols[jj]={t:v for t,v in new.items()}
        row=rowb(tiles[t0],s0)
        row=jnp.where(lane==j,1.0,row)
        for t in range(t0,n):
            v=jnp.where(lane==j,0.0,tiles[t])-M[t]*row
            if t==t0: v=jnp.where(below,v,tiles[t])
            tiles[t]=v
    return tiles


def assemble(pos_ref, own_ref, other_ref, w_ref):
    lane = lax.broadcasted_iota(jnp.int32, (256, B), 1)
    y, k = pos_ref[0], pos_ref[1]
    north = k == 0
    for q in range(4):
        ahead = lax.rem(q - y + 4, 4)

        def place(i, _):
            at = pl.ds(pl.multiple_of(i * 256, 256), 256)
            mine, theirs = own_ref[ahead, at, :], other_ref[ahead, at, :]
            low = jnp.where(north, mine, theirs)
            high = jnp.where(north, theirs, mine)
            w_ref[at, q * B : (q + 1) * B] = jnp.where(lane < 64, low, pltpu.roll(high, 64, 1))
            w_ref[at, 512 + q * B : 512 + (q + 1) * B] = jnp.where(
                lane < 64, pltpu.roll(low, 64, 1), high
            )
            return 0

        lax.fori_loop(0, 4, place, 0)


def factor_steps(w_ref, d_ref, left_ref, first, last):
    lane8 = lax.broadcasted_iota(jnp.int32, (8, B), 1)
    r = lax.broadcasted_iota(jnp.int32, (B, B), 0)
    c = lax.broadcasted_iota(jnp.int32, (B, B), 1)

    def step(k, _):
        ks = pl.ds(pl.multiple_of(k * B, B), B)
        block = w_ref[ks, ks]
        tiles = eliminate([block[8 * t : 8 * t + 8, :] for t in range(B // 8)], lane8)
        whole = jnp.concatenate(tiles, 0)
        pivots = jnp.sum(jnp.where(r == c, whole, 0.0), axis=1, keepdims=True)
        inverse = jnp.where(r == c, 1.0, jnp.where(r > c, whole, 0.0)) * lax.rsqrt(pivots)
        d_ref[...] = inverse
        w_ref[ks, :] = mm(inverse, w_ref[ks, :])
        w_ref[ks, ks] = inverse

        below = lax.broadcasted_iota(jnp.int32, (LEAD, B), 0) // B > k
        column = w_ref[:, ks]
        left_ref[...] = mm(
            jnp.where(below, column, 0.0), d_ref[...], (((1,), (1,)), ((), ()))
        )
        w_ref[:, ks] = jnp.where(below, 0.0, column)

        def update(i, _):
            at = pl.ds(pl.multiple_of(i * 256, 256), 256)
            w_ref[at, :] = w_ref[at, :] - mm(left_ref[at, :], w_ref[ks, :])
            return 0

        lax.fori_loop((k + 1) // 2, 4, update, 0)
        return 0

    lax.fori_loop(first, last, step, 0)


def first_kernel(pos_ref, own_ref, other_ref, w_ref, d_ref, left_ref):
    assemble(pos_ref, own_ref, other_ref, w_ref)
    factor_steps(w_ref, d_ref, left_ref, 0, FIRST)


def second_kernel(in_ref, w_ref, d_ref, left_ref):
    w_ref[...] = in_ref[...]
    factor_steps(w_ref, d_ref, left_ref, FIRST, 8)
    block = lax.broadcasted_iota(jnp.int32, (B, LEAD), 1) // B
    for k in range(8):
        w_ref[k * B : (k + 1) * B, :] = jnp.where(block <= k, w_ref[k * B : (k + 1) * B, :], 0.0)


def factor_call(body, inputs, specs, name):
    return pl.pallas_call(
        body,
        out_shape=jax.ShapeDtypeStruct((LEAD, LEAD), jnp.float32),
        in_specs=specs,
        out_specs=VMEM,
        scratch_shapes=[pltpu.VMEM((B, B), jnp.float32), pltpu.VMEM((LEAD, B), jnp.float32)],
        cost_estimate=pl.CostEstimate(
            flops=20_000_000_000, bytes_accessed=8_000_000, transcendentals=0
        ),
        compiler_params=pltpu.CompilerParams(vmem_limit_bytes=40 * 1024 * 1024),
        name=name,
    )(*inputs)


def gram_kernel(pos_ref, x_ref, *refs):
    own, other, out_ref, held = refs[:4], refs[4:8], refs[8], refs[9]
    step = pl.program_id(0)
    for d in range(4):

        @pl.when(step == d)
        def _():
            held[0] = own[d][...]
            held[1] = other[d][...]

    k = pos_ref[1] ^ pos_ref[5]
    total = jnp.dot(held[0], x_ref[0, k], preferred_element_type=jnp.float32)
    total += jnp.dot(held[1], x_ref[0, 1 - k], preferred_element_type=jnp.float32)

    @pl.when(step == 0)
    def _():
        out_ref[...] = total

    @pl.when(step > 0)
    def _():
        out_ref[...] += total


def gram(pos, x, own, other):
    feats, block = own[0].shape
    width = x.shape[-1]
    whole = pl.BlockSpec((feats, block), lambda i, pos: (0, 0))
    return pl.pallas_call(
        gram_kernel,
        out_shape=jax.ShapeDtypeStruct((feats, width), jnp.float32),
        grid_spec=pltpu.PrefetchScalarGridSpec(
            num_scalar_prefetch=1,
            grid=(4,),
            in_specs=[
                pl.BlockSpec(
                    (1, 2, block, width), lambda i, pos: (lax.rem(pos[0] + i, 4) ^ pos[4], 0, 0, 0)
                )
            ]
            + [whole] * 8,
            out_specs=pl.BlockSpec((feats, width), lambda i, pos: (0, 0)),
            scratch_shapes=[pltpu.VMEM((2, feats, block), jnp.bfloat16)],
        ),
        cost_estimate=pl.CostEstimate(
            flops=6_600_000_000, bytes_accessed=24_000_000, transcendentals=0
        ),
        compiler_params=pltpu.CompilerParams(vmem_limit_bytes=48 * 1024 * 1024),
        name="gram",
    )(pos, x, *own, *other)


def triangular_product(pos_ref, inv_ref, held, out_ref, masked):
    width = out_ref.shape[1]
    lane = lax.broadcasted_iota(jnp.int32, (B, width), 1)
    for i in range(8):
        depth = (i + 1) * B
        value = mm(inv_ref[i * B : depth, :depth], held[:depth, :])
        if i >= 4:
            value = jnp.where((lane < TILE) & masked, 0.0, value)
        out_ref[i * B : depth, :] = value


def panel_col_kernel(pos_ref, inv_ref, *refs):
    pieces, out_ref, held = refs[:4], refs[4], refs[5]
    y, k = pos_ref[0], pos_ref[1]
    for d in range(4):
        for side in range(2):
            row = lax.rem(y + d, 4) * 2 + (1 - k if side else k)
            for t in range(2):
                at = pl.ds(pl.multiple_of(t * 512 + row * TILE, TILE), TILE)
                held[at, :] = pieces[d][side, t * TILE : (t + 1) * TILE, :]
    triangular_product(pos_ref, inv_ref, held, out_ref, pos_ref[2] < 2)


def panel_row_kernel(pos_ref, inv_ref, *refs):
    left, right, out_ref, held = refs[:4], refs[4:8], refs[8], refs[9]
    z, x = pos_ref[2], pos_ref[3]
    for i in range(4):
        for j in range(4):
            col = lax.rem(z + i, 4) * 4 + lax.rem(x + j, 4)
            at = pl.ds(pl.multiple_of(col * TILE, TILE), TILE)
            held[at, :SPLIT] = left[i][j]
            held[at, SPLIT:] = right[j][i]
    triangular_product(pos_ref, inv_ref, held, out_ref, True)


def panel_call(body, pos, inverse, pieces, width, name):
    return pl.pallas_call(
        body,
        out_shape=jax.ShapeDtypeStruct((LEAD, width), jnp.float32),
        in_specs=[SMEM] + [VMEM] * (1 + len(pieces)),
        out_specs=VMEM,
        scratch_shapes=[pltpu.VMEM((LEAD, width), jnp.float32)],
        cost_estimate=pl.CostEstimate(
            flops=LEAD * LEAD * width * 6, bytes_accessed=12_000_000, transcendentals=0
        ),
        compiler_params=pltpu.CompilerParams(vmem_limit_bytes=40 * 1024 * 1024),
        name=name,
    )(pos, inverse, *pieces)


def fetch(x, axis, ahead):
    size = lax.axis_size(axis)
    return lax.ppermute(x, axis, [(i, (i - ahead) % size) for i in range(size)])


def fetch_each(x, axis):
    return [x] + [fetch(x, axis, ahead) for ahead in (1, 2, 3)]


def swap(x):
    return fetch(x, "row_k", 1)


def copy_for_each(x, axes, size):
    return lax.all_to_all(jnp.broadcast_to(x[None], (size, *x.shape)), axes, 0, 0, tiled=True)


def fetch_shares(x, axis):
    me = lax.axis_index(axis)
    return [lax.dynamic_index_in_dim(x, me, 0, keepdims=False)] + [
        fetch(lax.dynamic_index_in_dim(x, (me - ahead) % 4, 0, keepdims=False), axis, ahead)
        for ahead in (1, 2, 3)
    ]


def column_features_to_send(activations, row, col):
    tokens, width = activations.shape
    turned = activations.T.reshape(-1, 2, TILE, tokens)
    halves = [turned[:, h].reshape(width // 2, tokens) for h in range(2)]
    odd = col % 2 == 1
    sent = [jnp.where(odd, halves[1], halves[0]), jnp.where(odd, halves[0], halves[1])]
    pairs = [[], []]
    for other in range(2):
        for i in range(128):
            s, c = i // 16, i % 16
            pairs[other].append((i, ((c // 2) ^ s) * 16 + s + 8 * ((c % 2) ^ other)))
    return sent, pairs


def dot0(left, right):
    return lax.dot_general(
        left, right, (((0,), (0,)), ((), ())), preferred_element_type=jnp.float32
    )


def dot0_high(left, right):
    return lax.dot_general(
        left, right, (((0,), (0,)), ((), ())), precision=lax.Precision.HIGHEST
    )


def on_device(activations, running, deltas, samples):
    y, k = lax.axis_index("row_y"), lax.axis_index("row_k")
    z, x = lax.axis_index("col_0"), lax.axis_index("col_1")
    row, col = y * 2 + k, z * 4 + x
    pos = jnp.stack([y, k, z, x, z % 2 * 2 + x // 2, x % 2]).astype(jnp.int32)
    rows, cols = running.shape
    row_local = jnp.arange(rows, dtype=jnp.int32)
    col_local = jnp.arange(cols, dtype=jnp.int32)
    row_global = (row_local // TILE * 8 + row) * TILE + row_local % TILE
    col_global = (col_local // TILE * 16 + col) * TILE + col_local % TILE

    everything = lax.all_gather(activations, COL, axis=0)
    everything = with_layout_constraint(everything, Layout((0, 1, 2)))
    tokens = everything.shape[0] * everything.shape[1]
    scale = (1.0 - DECAY) / tokens

    lead = activations[:, :128]

    lead_all = copy_for_each(lead, ROW, 8)
    partial = lax.dot_general(
        lead_all, lead, (((1,), (0,)), ((), ())), preferred_element_type=jnp.float32
    )
    partial = partial.reshape(8, 2, TILE, 128).swapaxes(0, 1).reshape(16, TILE, 128)
    lead_sum = lax.all_to_all(partial, COL, 0, 0, tiled=True).sum(0)
    same = (row_global[None, :128] == col_global[:TILE, None]).astype(jnp.float32)
    lead_t = DECAY * running[:128, :TILE].T + scale * lead_sum + DAMPING * same
    lead_cols = copy_for_each(lead_t, COL, 16).reshape(LEAD, 128)
    parts = jnp.stack(fetch_each(lead_cols, "row_y"))

    weights = (samples.astype(jnp.float32) / SHOTS).astype(jnp.bfloat16)
    partial_t = jnp.einsum(
        "k,kmn->nm", weights, deltas, preferred_element_type=jnp.float32
    )
    sent, pairs = column_features_to_send(activations, row, col)
    sent, partial_t, parts = lax.optimization_barrier((sent, partial_t, parts))
    other_parts = swap(parts)
    sent, parts, other_parts = lax.optimization_barrier((sent, parts, other_parts))
    got = [lax.ppermute(part, ALL, pair) for part, pair in zip(sent, pairs)]
    slab_parts = fetch_shares(partial_t.reshape(4, 64, rows), "col_0")
    state = factor_call(first_kernel, (pos, parts, other_parts), [SMEM, VMEM, VMEM], "factor_a")

    got, slab_parts, state = lax.optimization_barrier((got, slab_parts, state))
    high = col // 8 == 1
    feats = jnp.concatenate(
        [jnp.where(high, got[1], got[0]), jnp.where(high, got[0], got[1])], 1
    )
    y_own = fetch_each(feats, "row_y")
    slab_parts = fetch_shares(sum(slab_parts).reshape(4, 16, rows), "col_1")
    inverse = factor_call(second_kernel, (state,), [VMEM], "factor_b")

    y_own, slab_parts, inverse = lax.optimization_barrier((y_own, slab_parts, inverse))
    y_other = [swap(part) for part in y_own]
    slab_t = sum(slab_parts)
    slab_side = jnp.stack([slab_t[:, :128], swap(slab_t[:, :128])])
    slab_lead = fetch_each(slab_side, "row_y")
    by_block = everything.reshape(4, 2, tokens // 8, rows)
    gram_t = gram(pos, by_block, y_own, y_other)
    slab_lead, gram_t = lax.optimization_barrier((slab_lead, gram_t))

    diag_t = (row_global[None, :] == col_global[:TILE, None]).astype(jnp.float32)
    e_mine = DECAY * running[:, :TILE].T + scale * gram_t[:TILE] + DAMPING * diag_t
    diag_lead = (row_global[:128, None] == col_global[None, :]).astype(jnp.float32)
    top = DECAY * running[:128] + scale * gram_t[:, :128].T + DAMPING * diag_lead
    left = jnp.stack(fetch_each(e_mine[:, :SPLIT], "col_1"))
    right = jnp.stack(fetch_each(e_mine[:, SPLIT:], "col_0"))
    top_sides = jnp.stack([top, swap(top)])
    left, right, top_sides = lax.optimization_barrier((left, right, top_sides))
    left = fetch_each(left, "col_0")
    right = fetch_each(right, "col_1")
    top_sides = fetch_each(top_sides, "row_y")

    diag = (row_global[:, None] == col_global[None, :]).astype(jnp.float32)
    factor = DECAY * running + scale * gram_t.T + DAMPING * diag

    panel_col = panel_call(panel_col_kernel, pos, inverse, top_sides, cols, "panel_col")
    panel_row = panel_call(panel_row_kernel, pos, inverse, left + right, rows, "panel_row")
    updated = factor - dot0_high(panel_row, panel_col)
    panel_out = lax.dynamic_slice_in_dim(panel_row, col * TILE, TILE, 0).T

    slab_lead = jnp.stack(slab_lead)
    slab_lead = jnp.where(k == 0, slab_lead, slab_lead[:, ::-1])
    slab_lead = jnp.roll(slab_lead, y, axis=0)
    slab_lead = slab_lead.reshape(4, 2, 16, 2, TILE).transpose(2, 3, 0, 1, 4).reshape(16, LEAD)
    head = lax.dot_general(
        slab_lead, inverse, (((1,), (1,)), ((), ())), precision=lax.Precision.HIGHEST
    )
    own_head = lax.dynamic_index_in_dim(
        head.reshape(16, 2, 8, TILE), row, 2, keepdims=False
    ).reshape(16, 128)
    rest = jnp.dot(head, panel_row, precision=lax.Precision.HIGHEST)
    solved = jnp.concatenate([own_head, slab_t[:, 128:] - rest[:, 128:]], 1).T
    return updated, panel_out, solved


def solution(mesh):
    finer = Mesh(mesh.devices.reshape(4, 2, 4, 4), ("row_y", "row_k", "col_0", "col_1"))
    return jax.shard_map(
        on_device,
        mesh=finer,
        in_specs=(P(COL, ROW), P(ROW, COL), P(COL, ROW, None), P(COL)),
        out_specs=(P(ROW, COL), P(ROW, COL), P(ROW, COL)),
        check_vma=False,
    )
```

```python
import jax
import jax.numpy as jnp
from jax import lax
from jax.experimental import pallas as pl
from jax.experimental.layout import Layout, with_layout_constraint
from jax.experimental.pallas import tpu as pltpu
from jax.sharding import Mesh
from jax.sharding import PartitionSpec as P

TILE = 64
SHOTS = 64
LEAD = 1024
DECAY = 0.75
DAMPING = 0.05
COL = ("col_0", "col_1")
ROW = ("row_y", "row_k")
ALL = ROW + COL
B = 128
DEPTH = 5
FIRST = 3
SPLIT = 512
VMEM = pl.BlockSpec(memory_space=pltpu.VMEM)
SMEM = pl.BlockSpec(memory_space=pltpu.SMEM)


def mm(a,b,dims=(((1,),(0,)),((),()))):
    return lax.dot_general(a,b,dims,precision=lax.Precision.HIGHEST,preferred_element_type=jnp.float32)

def eliminate(tiles, lane):
    n=len(tiles)
    sub=lax.broadcasted_iota(jnp.int32,(8,128),0)
    def bc(x,j): return jnp.broadcast_to(x[:, j:j+1],(8,128))
    def rowb(x,i): return jnp.broadcast_to(x[i:i+1,:],(8,128))
    cols={}
    for j in range(min(DEPTH,B)):
        cols[j]={t:bc(tiles[t],j) for t in range(j//8,n)}
    for j in range(B):
        t0,s0=j//8,j%8
        jn=j+DEPTH
        if jn<B:
            cols[jn]={t:bc(tiles[t],jn) for t in range(t0,n)}
        C=cols.pop(j)
        piv=rowb(C[t0],s0)
        rinv=1.0/piv
        M={t:C[t]*rinv for t in range(t0,n)}
        below=sub>s0
        for jj in range(j+1,min(jn,B-1)+1):
            cj=cols[jj]
            f=rowb(cj[t0],s0)
            new={}
            for t in range(t0,n):
                if t<jj//8 and t!=t0: pass
                v=cj[t]-M[t]*f
                if t==t0: v=jnp.where(below,v,cj[t])
                new[t]=v
            cols[jj]={t:v for t,v in new.items()}
        row=rowb(tiles[t0],s0)
        row=jnp.where(lane==j,1.0,row)
        for t in range(t0,n):
            v=jnp.where(lane==j,0.0,tiles[t])-M[t]*row
            if t==t0: v=jnp.where(below,v,tiles[t])
            tiles[t]=v
    return tiles


def assemble(pos_ref, own_ref, other_ref, w_ref):
    lane = lax.broadcasted_iota(jnp.int32, (256, B), 1)
    y, k = pos_ref[0], pos_ref[1]
    north = k == 0
    for q in range(4):
        ahead = lax.rem(q - y + 4, 4)

        def place(i, _):
            at = pl.ds(pl.multiple_of(i * 256, 256), 256)
            mine, theirs = own_ref[ahead, at, :], other_ref[ahead, at, :]
            low = jnp.where(north, mine, theirs)
            high = jnp.where(north, theirs, mine)
            w_ref[at, q * B : (q + 1) * B] = jnp.where(lane < 64, low, pltpu.roll(high, 64, 1))
            w_ref[at, 512 + q * B : 512 + (q + 1) * B] = jnp.where(
                lane < 64, pltpu.roll(low, 64, 1), high
            )
            return 0

        lax.fori_loop(0, 4, place, 0)


def factor_steps(w_ref, d_ref, left_ref, first, last):
    lane8 = lax.broadcasted_iota(jnp.int32, (8, B), 1)
    r = lax.broadcasted_iota(jnp.int32, (B, B), 0)
    c = lax.broadcasted_iota(jnp.int32, (B, B), 1)

    def step(k, _):
        ks = pl.ds(pl.multiple_of(k * B, B), B)
        block = w_ref[ks, ks]
        tiles = eliminate([block[8 * t : 8 * t + 8, :] for t in range(B // 8)], lane8)
        whole = jnp.concatenate(tiles, 0)
        pivots = jnp.sum(jnp.where(r == c, whole, 0.0), axis=1, keepdims=True)
        inverse = jnp.where(r == c, 1.0, jnp.where(r > c, whole, 0.0)) * lax.rsqrt(pivots)
        d_ref[...] = inverse
        w_ref[ks, :] = mm(inverse, w_ref[ks, :])
        w_ref[ks, ks] = inverse

        below = lax.broadcasted_iota(jnp.int32, (LEAD, B), 0) // B > k
        column = w_ref[:, ks]
        left_ref[...] = mm(
            jnp.where(below, column, 0.0), d_ref[...], (((1,), (1,)), ((), ()))
        )
        w_ref[:, ks] = jnp.where(below, 0.0, column)

        def update(i, _):
            at = pl.ds(pl.multiple_of(i * 256, 256), 256)
            w_ref[at, :] = w_ref[at, :] - mm(left_ref[at, :], w_ref[ks, :])
            return 0

        lax.fori_loop((k + 1) // 2, 4, update, 0)
        return 0

    lax.fori_loop(first, last, step, 0)


def first_kernel(pos_ref, own_ref, other_ref, w_ref, d_ref, left_ref):
    assemble(pos_ref, own_ref, other_ref, w_ref)
    factor_steps(w_ref, d_ref, left_ref, 0, FIRST)


def second_kernel(in_ref, w_ref, d_ref, left_ref):
    w_ref[...] = in_ref[...]
    factor_steps(w_ref, d_ref, left_ref, FIRST, 8)
    block = lax.broadcasted_iota(jnp.int32, (B, LEAD), 1) // B
    for k in range(8):
        w_ref[k * B : (k + 1) * B, :] = jnp.where(block <= k, w_ref[k * B : (k + 1) * B, :], 0.0)


def factor_call(body, inputs, specs, name):
    return pl.pallas_call(
        body,
        out_shape=jax.ShapeDtypeStruct((LEAD, LEAD), jnp.float32),
        in_specs=specs,
        out_specs=VMEM,
        scratch_shapes=[pltpu.VMEM((B, B), jnp.float32), pltpu.VMEM((LEAD, B), jnp.float32)],
        cost_estimate=pl.CostEstimate(
            flops=20_000_000_000, bytes_accessed=8_000_000, transcendentals=0
        ),
        compiler_params=pltpu.CompilerParams(vmem_limit_bytes=40 * 1024 * 1024),
        name=name,
    )(*inputs)


def gram_kernel(pos_ref, x_ref, *refs):
    own, other, out_ref, held = refs[:4], refs[4:8], refs[8], refs[9]
    step = pl.program_id(0)
    for d in range(4):

        @pl.when(step == d)
        def _():
            held[0] = own[d][...]
            held[1] = other[d][...]

    k = pos_ref[1] ^ pos_ref[5]
    total = jnp.dot(held[0], x_ref[0, k], preferred_element_type=jnp.float32)
    total += jnp.dot(held[1], x_ref[0, 1 - k], preferred_element_type=jnp.float32)

    @pl.when(step == 0)
    def _():
        out_ref[...] = total

    @pl.when(step > 0)
    def _():
        out_ref[...] += total


def gram(pos, x, own, other):
    feats, block = own[0].shape
    width = x.shape[-1]
    whole = pl.BlockSpec((feats, block), lambda i, pos: (0, 0))
    return pl.pallas_call(
        gram_kernel,
        out_shape=jax.ShapeDtypeStruct((feats, width), jnp.float32),
        grid_spec=pltpu.PrefetchScalarGridSpec(
            num_scalar_prefetch=1,
            grid=(4,),
            in_specs=[
                pl.BlockSpec(
                    (1, 2, block, width), lambda i, pos: (lax.rem(pos[0] + i, 4) ^ pos[4], 0, 0, 0)
                )
            ]
            + [whole] * 8,
            out_specs=pl.BlockSpec((feats, width), lambda i, pos: (0, 0)),
            scratch_shapes=[pltpu.VMEM((2, feats, block), jnp.bfloat16)],
        ),
        cost_estimate=pl.CostEstimate(
            flops=6_600_000_000, bytes_accessed=24_000_000, transcendentals=0
        ),
        compiler_params=pltpu.CompilerParams(vmem_limit_bytes=48 * 1024 * 1024),
        name="gram",
    )(pos, x, *own, *other)


def triangular_product(pos_ref, inv_ref, held, out_ref, masked):
    width = out_ref.shape[1]
    lane = lax.broadcasted_iota(jnp.int32, (B, width), 1)
    for i in range(8):
        depth = (i + 1) * B
        value = mm(inv_ref[i * B : depth, :depth], held[:depth, :])
        if i >= 4:
            value = jnp.where((lane < TILE) & masked, 0.0, value)
        out_ref[i * B : depth, :] = value


def panel_col_kernel(pos_ref, inv_ref, *refs):
    pieces, out_ref, held = refs[:2], refs[2], refs[3]
    y, k = pos_ref[0], pos_ref[1]
    for d in range(4):
        for side in range(2):
            row = lax.rem(y + d, 4) * 2 + (1 - k if side else k)
            for t in range(2):
                at = pl.ds(pl.multiple_of(t * 512 + row * TILE, TILE), TILE)
                held[at, :] = pieces[side][d, t * TILE : (t + 1) * TILE, :]
    triangular_product(pos_ref, inv_ref, held, out_ref, pos_ref[2] < 2)


def panel_row_kernel(pos_ref, inv_ref, *refs):
    left, right, out_ref, held = refs[:4], refs[4:8], refs[8], refs[9]
    z, x = pos_ref[2], pos_ref[3]
    for i in range(4):
        for j in range(4):
            col = lax.rem(z + i, 4) * 4 + lax.rem(x + j, 4)
            at = pl.ds(pl.multiple_of(col * TILE, TILE), TILE)
            held[at, :SPLIT] = left[i][j]
            held[at, SPLIT:] = right[j][i]
    triangular_product(pos_ref, inv_ref, held, out_ref, True)


def panel_call(body, pos, inverse, pieces, width, name):
    return pl.pallas_call(
        body,
        out_shape=jax.ShapeDtypeStruct((LEAD, width), jnp.float32),
        in_specs=[SMEM] + [VMEM] * (1 + len(pieces)),
        out_specs=VMEM,
        scratch_shapes=[pltpu.VMEM((LEAD, width), jnp.float32)],
        cost_estimate=pl.CostEstimate(
            flops=LEAD * LEAD * width * 6, bytes_accessed=12_000_000, transcendentals=0
        ),
        compiler_params=pltpu.CompilerParams(vmem_limit_bytes=40 * 1024 * 1024),
        name=name,
    )(pos, inverse, *pieces)


def fetch(x, axis, ahead):
    size = lax.axis_size(axis)
    return lax.ppermute(x, axis, [(i, (i - ahead) % size) for i in range(size)])


def fetch_each(x, axis):
    return [x] + [fetch(x, axis, ahead) for ahead in (1, 2, 3)]


def swap(x):
    return fetch(x, "row_k", 1)


def copy_for_each(x, axes, size):
    return lax.all_to_all(jnp.broadcast_to(x[None], (size, *x.shape)), axes, 0, 0, tiled=True)


def fetch_shares(x, axis):
    me = lax.axis_index(axis)
    return [lax.dynamic_index_in_dim(x, me, 0, keepdims=False)] + [
        fetch(lax.dynamic_index_in_dim(x, (me - ahead) % 4, 0, keepdims=False), axis, ahead)
        for ahead in (1, 2, 3)
    ]


def column_features_to_send(activations, row, col):
    tokens, width = activations.shape
    turned = activations.T.reshape(-1, 2, TILE, tokens)
    halves = [turned[:, h].reshape(width // 2, tokens) for h in range(2)]
    odd = col % 2 == 1
    sent = [jnp.where(odd, halves[1], halves[0]), jnp.where(odd, halves[0], halves[1])]
    pairs = [[], []]
    for other in range(2):
        for i in range(128):
            s, c = i // 16, i % 16
            pairs[other].append((i, ((c // 2) ^ s) * 16 + s + 8 * ((c % 2) ^ other)))
    return sent, pairs


def dot0(left, right):
    return lax.dot_general(
        left, right, (((0,), (0,)), ((), ())), preferred_element_type=jnp.float32
    )


def dot0_high(left, right):
    return lax.dot_general(
        left, right, (((0,), (0,)), ((), ())), precision=lax.Precision.HIGHEST
    )


def on_device(activations, running, deltas, samples):
    y, k = lax.axis_index("row_y"), lax.axis_index("row_k")
    z, x = lax.axis_index("col_0"), lax.axis_index("col_1")
    row, col = y * 2 + k, z * 4 + x
    pos = jnp.stack([y, k, z, x, z % 2 * 2 + x // 2, x % 2]).astype(jnp.int32)
    rows, cols = running.shape
    row_local = jnp.arange(rows, dtype=jnp.int32)
    col_local = jnp.arange(cols, dtype=jnp.int32)
    row_global = (row_local // TILE * 8 + row) * TILE + row_local % TILE
    col_global = (col_local // TILE * 16 + col) * TILE + col_local % TILE

    tokens = activations.shape[0] * 16
    scale = (1.0 - DECAY) / tokens

    lead = activations[:, :128]

    lead_all = copy_for_each(lead, ROW, 8)
    partial = lax.dot_general(
        lead_all, lead, (((1,), (0,)), ((), ())), preferred_element_type=jnp.float32
    )
    partial = partial.reshape(8, 2, TILE, 128).swapaxes(0, 1).reshape(16, TILE, 128)
    lead_sum = lax.all_to_all(partial, COL, 0, 0, tiled=True).sum(0)
    same = (row_global[None, :128] == col_global[:TILE, None]).astype(jnp.float32)
    lead_t = DECAY * running[:128, :TILE].T + scale * lead_sum + DAMPING * same
    lead_cols = copy_for_each(lead_t, COL, 16).reshape(LEAD, 128)

    activations, lead_cols = lax.optimization_barrier((activations, lead_cols))
    everything = lax.all_gather(activations, COL, axis=0)
    everything = with_layout_constraint(everything, Layout((0, 1, 2)))

    parts = jnp.stack(fetch_each(lead_cols, "row_y"))

    weights = (samples.astype(jnp.float32) / SHOTS).astype(jnp.bfloat16)
    partial_t = jnp.einsum(
        "k,kmn->nm", weights, deltas, preferred_element_type=jnp.float32
    )
    sent, pairs = column_features_to_send(activations, row, col)
    sent, partial_t, parts = lax.optimization_barrier((sent, partial_t, parts))
    other_parts = swap(parts)
    sent, parts, other_parts = lax.optimization_barrier((sent, parts, other_parts))
    got = [lax.ppermute(part, ALL, pair) for part, pair in zip(sent, pairs)]
    slab_parts = fetch_shares(partial_t.reshape(4, 64, rows), "col_0")
    state = factor_call(first_kernel, (pos, parts, other_parts), [SMEM, VMEM, VMEM], "factor_a")

    got, slab_parts, state = lax.optimization_barrier((got, slab_parts, state))
    high = col // 8 == 1
    feats = jnp.concatenate(
        [jnp.where(high, got[1], got[0]), jnp.where(high, got[0], got[1])], 1
    )
    y_own = fetch_each(feats, "row_y")
    slab_parts = fetch_shares(sum(slab_parts).reshape(4, 16, rows), "col_1")
    inverse = factor_call(second_kernel, (state,), [VMEM], "factor_b")

    y_own, slab_parts, inverse = lax.optimization_barrier((y_own, slab_parts, inverse))
    y_other = [swap(part) for part in y_own]
    slab_t = sum(slab_parts)
    slab_side = jnp.stack([slab_t[:, :128], swap(slab_t[:, :128])])
    by_block = everything.reshape(4, 2, tokens // 8, rows)
    gram_t = gram(pos, by_block, y_own, y_other)
    slab_side, gram_t = lax.optimization_barrier((slab_side, gram_t))

    diag_t = (row_global[None, :] == col_global[:TILE, None]).astype(jnp.float32)
    e_mine = DECAY * running[:, :TILE].T + scale * gram_t[:TILE] + DAMPING * diag_t
    diag_lead = (row_global[:128, None] == col_global[None, :]).astype(jnp.float32)
    top = DECAY * running[:128] + scale * gram_t[:, :128].T + DAMPING * diag_lead
    left = jnp.stack(fetch_each(e_mine[:, :SPLIT], "col_1"))
    right = jnp.stack(fetch_each(e_mine[:, SPLIT:], "col_0"))
    top_own = jnp.stack(fetch_each(top, "row_y"))
    left, right, top_own, slab_side = lax.optimization_barrier((left, right, top_own, slab_side))
    top_other = swap(top_own)
    left = fetch_each(left, "col_0")
    right = fetch_each(right, "col_1")
    slab_lead = fetch_each(slab_side, "row_y")

    diag = (row_global[:, None] == col_global[None, :]).astype(jnp.float32)
    factor = DECAY * running + scale * gram_t.T + DAMPING * diag

    panel_col = panel_call(panel_col_kernel, pos, inverse, (top_own, top_other), cols, "panel_col")
    panel_row = panel_call(panel_row_kernel, pos, inverse, left + right, rows, "panel_row")
    updated = factor - dot0_high(panel_row, panel_col)
    panel_out = lax.dynamic_slice_in_dim(panel_row, col * TILE, TILE, 0).T

    slab_lead = jnp.stack(slab_lead)
    slab_lead = jnp.where(k == 0, slab_lead, slab_lead[:, ::-1])
    slab_lead = jnp.roll(slab_lead, y, axis=0)
    slab_lead = slab_lead.reshape(4, 2, 16, 2, TILE).transpose(2, 3, 0, 1, 4).reshape(16, LEAD)
    head = lax.dot_general(
        slab_lead, inverse, (((1,), (1,)), ((), ())), precision=lax.Precision.HIGHEST
    )
    own_head = lax.dynamic_index_in_dim(
        head.reshape(16, 2, 8, TILE), row, 2, keepdims=False
    ).reshape(16, 128)
    rest = jnp.dot(head, panel_row, precision=lax.Precision.HIGHEST)
    solved = jnp.concatenate([own_head, slab_t[:, 128:] - rest[:, 128:]], 1).T
    return updated, panel_out, solved


def solution(mesh):
    finer = Mesh(mesh.devices.reshape(4, 2, 4, 4), ("row_y", "row_k", "col_0", "col_1"))
    return jax.shard_map(
        on_device,
        mesh=finer,
        in_specs=(P(COL, ROW), P(ROW, COL), P(COL, ROW, None), P(COL)),
        out_specs=(P(ROW, COL), P(ROW, COL), P(ROW, COL)),
        check_vma=False,
    )
```
